128 devices in a mesh: ctx: 16 (over z, x), bulk: 8 (over y, core).
Axes of the slice: x: 4, y: 4, z: 4, core: 2. Of those that a mesh axis runs over, the one named last changes fastest.
Arguments:
- query: bfloat16 [32768, 5120], P(('ctx', 'bulk')), may hold values from -1 to 1
- keys: bfloat16 [32768, 1024], P(('ctx', 'bulk')), may hold values from -1 to 1
- values: bfloat16 [32768, 1024], P(('ctx', 'bulk')), may hold values from -6 to 6
- output: bfloat16 [32768, 5120], P(('ctx', 'bulk')), may hold values from -3 to 3
- grad_out: bfloat16 [32768, 5120], P(('ctx', 'bulk')), may hold values from -12 to 12
- logsumexp: float32 [32768, 40], P(('ctx', 'bulk')), may hold values from 3 to 5
- selected: int32 [256, 8, 3], P(('ctx', 'bulk')), may hold values from -1 to 255, as said below
Outputs:
- grad_query: bfloat16 [32768, 5120], P(('ctx', 'bulk'))
- grad_keys: bfloat16 [32768, 1024], P(('ctx', 'bulk'))
- grad_values: bfloat16 [32768, 1024], P(('ctx', 'bulk'))
The draws below stay inside these ranges and needn't reach their ends.
Inputs may be any that keep to these rules, and one draw needn't show every extreme that they name: `selected`: entry [b, h, s] is -1 (no block) or a block on a device before the device of block b. Over all entries of one device's 2 blocks, each other device is named at most once; a device with 48 or more devices before it has no -1. Every device but the first names the device just before it, and the last device names the first device.
All inputs are finite; a program needn't handle non-finite values.
Results may differ from the reference program's by a relative error of at most 0.0062.
Values may be sent and summed in bfloat16 or wider, within the bound.
A program may use at most 192 MiB of HBM per device.

```python
import jax
import jax.numpy as jnp
from jax import lax

HD = 128
KVH = 8
GROUP = 5
QH = 40
BLK = 128
TOPK = 3
BPD = 2
TOKENS = 32768
BLOCKS = 256
DEVICES = 128


def draw_selected(key, part):
    count_peers = DEVICES
    per_device = BPD * KVH * TOPK
    width = count_peers + per_device
    first, second, third, fourth = jax.random.split(jax.random.fold_in(key, 17), 4)
    noise = jax.random.randint(first, (count_peers, width), 0, 65536)
    favour = jax.random.randint(second, (width,), 0, 4)
    columns = jnp.arange(width, dtype=jnp.int32)
    device_ids = jnp.arange(count_peers, dtype=jnp.int32)[:, None]
    base = (noise + favour[None, :] * 32768) * width + columns[None, :]
    forced = (columns[None, :] == device_ids - 1) | (columns[None, :] == 0) & (device_ids == count_peers - 1)
    base = jnp.where(forced, 1073741824 + columns[None, :], base)
    score = jnp.where(columns[None, :] < device_ids, base, -1 - columns[None, :])
    _, picked = lax.top_k(score, per_device)
    ranks = jnp.arange(per_device, dtype=jnp.int32)[None, :]
    usable = ranks < jnp.minimum(device_ids, per_device)
    order_keys = jax.random.randint(third, (count_peers, per_device), 0, 65536) * per_device + ranks
    shuffle = jnp.argsort(order_keys, axis=1)
    owners = jnp.take_along_axis(picked, shuffle, axis=1)
    usable = jnp.take_along_axis(usable, shuffle, axis=1)
    within = jax.random.randint(fourth, (count_peers, per_device), 0, BPD)
    chosen = jnp.where(usable, owners * BPD + within, -1)
    return chosen.reshape(count_peers * BPD, KVH, TOPK).astype(jnp.int32)


def levels(own_key, extent, cuts, least, top_value):
    gain, own = 1.0, jax.random.fold_in(own_key, 6)
    for axis_at, shards_of in cuts:
        heights = jnp.exp(jax.random.uniform(jax.random.fold_in(own, axis_at), (shards_of,), jnp.float32, least / len(cuts), top_value / len(cuts)))
        gain = gain * jnp.repeat(heights, extent[axis_at] // shards_of).reshape([-1 if axis == axis_at else 1 for axis in range(len(extent))])
    return gain


def normal_values(rng, extent, spread, reach, cuts=(), held_as=jnp.bfloat16):
    array = jax.random.normal(rng, extent, jnp.float32) * spread
    if len(cuts) > 0:
        array = levels(rng, extent, cuts, -0.22, 0.18) * array
    return jnp.clip(array, min=-reach, max=reach).astype(held_as)


def setup_inputs(seed: int = 0) -> dict:
    arg_keys = jax.random.split(jax.random.key(seed), 8)
    query = jnp.clip(jax.random.uniform(arg_keys[0], (TOKENS, QH * HD), jnp.float32, -1.0, 1.0) * levels(arg_keys[0], (TOKENS, QH * HD), ((0, 128),), -0.4, 0.0), -1.0, 1.0).astype(jnp.bfloat16)
    keys = jnp.clip(jax.random.uniform(arg_keys[1], (TOKENS, KVH * HD), jnp.float32, -1.0, 1.0) * levels(arg_keys[1], (TOKENS, KVH * HD), ((0, 128),), -0.4, 0.0), -1.0, 1.0).astype(jnp.bfloat16)
    values = normal_values(arg_keys[2], (TOKENS, KVH * HD), 1.0, 6.0, ((0, 128),))
    output = normal_values(arg_keys[3], (TOKENS, QH * HD), 0.5, 3.0, ((0, 128),))
    grad_out = normal_values(arg_keys[4], (TOKENS, QH * HD), 2.0, 12.0, ((0, 128),))
    logsumexp = jnp.clip(3.0 + 2.0 * jax.random.uniform(arg_keys[5], (TOKENS, QH), jnp.float32) ** levels(arg_keys[5], (TOKENS, QH), ((0, 128),), -0.2, 0.2), 3.0, 5.0)
    selected = draw_selected(jax.random.fold_in(arg_keys[7], 71), 0)
    return dict(query=query, keys=keys, values=values, output=output, grad_out=grad_out, logsumexp=logsumexp, selected=selected)


def reference(query, keys, values, output, grad_out, logsumexp, selected):
    scale = HD ** -0.5
    high = lax.Precision.HIGHEST
    query_blocks = query.reshape(BLOCKS, BLK, KVH, GROUP, HD)
    grad_blocks = grad_out.reshape(BLOCKS, BLK, KVH, GROUP, HD)
    key_blocks = keys.reshape(BLOCKS, BLK, KVH, HD)
    value_blocks = values.reshape(BLOCKS, BLK, KVH, HD)
    delta = jnp.sum(grad_out.astype(jnp.float32).reshape(TOKENS, KVH, GROUP, HD)
                    * output.astype(jnp.float32).reshape(TOKENS, KVH, GROUP, HD), axis=-1)
    delta = delta.reshape(BLOCKS, BLK, KVH, GROUP)
    stats = logsumexp.reshape(BLOCKS, BLK, KVH, GROUP)
    heads = jnp.arange(KVH, dtype=jnp.int32)
    positions = jnp.arange(BLK, dtype=jnp.int32)
    causal = positions[None, :] <= positions[:, None]
    slot_ids = jnp.arange(TOPK + 1, dtype=jnp.int32)
    allowed = (slot_ids[None, :, None] > 0) | causal[:, None, :]

    def step(carry, index):
        key_acc, value_acc = carry
        chosen = jnp.concatenate([jnp.full((KVH, 1), index, jnp.int32), selected[index].astype(jnp.int32)], axis=1)
        usable = chosen >= 0
        safe = jnp.maximum(chosen, 0).astype(jnp.int32)
        key_set = key_blocks[safe, :, heads[:, None], :].astype(jnp.float32)
        value_set = value_blocks[safe, :, heads[:, None], :].astype(jnp.float32)
        queries = query_blocks[index].astype(jnp.float32)
        grads = grad_blocks[index].astype(jnp.float32)
        scores = jnp.einsum('qhgd,hjkd->hgqjk', queries, key_set, precision=high) * scale
        mask = usable[:, None, None, :, None] & allowed[None, None]
        logs = jnp.transpose(stats[index], (1, 2, 0))[..., None, None]
        probs32 = jnp.where(mask, jnp.exp(scores - logs), 0.0)
        probs = lax.optimization_barrier(probs32.astype(jnp.bfloat16)).astype(jnp.float32)
        value_part = jnp.einsum('hgqjk,qhgd->hjkd', probs, grads, precision=high)
        dprobs = jnp.einsum('qhgd,hjkd->hgqjk', grads, value_set, precision=high)
        shift = jnp.transpose(delta[index], (1, 2, 0))[..., None, None]
        dscores = lax.optimization_barrier((probs32 * (dprobs - shift)).astype(jnp.bfloat16)).astype(jnp.float32)
        query_grad = jnp.einsum('hgqjk,hjkd->qhgd', dscores, key_set, precision=high) * scale
        key_part = jnp.einsum('hgqjk,qhgd->hjkd', dscores, queries, precision=high) * scale
        key_acc = key_acc.at[safe, :, heads[:, None], :].add(key_part)
        value_acc = value_acc.at[safe, :, heads[:, None], :].add(value_part)
        return (key_acc, value_acc), query_grad.astype(jnp.bfloat16).reshape(BLK, KVH * GROUP * HD)

    zeros = jnp.zeros((BLOCKS, BLK, KVH, HD), jnp.float32)
    (key_acc, value_acc), query_grads = lax.scan(step, (zeros, zeros), jnp.arange(BLOCKS, dtype=jnp.int32))
    grad_query = query_grads.reshape(TOKENS, KVH * GROUP * HD)
    grad_keys = key_acc.reshape(TOKENS, KVH * HD).astype(jnp.bfloat16)
    grad_values = value_acc.reshape(TOKENS, KVH * HD).astype(jnp.bfloat16)
    return (grad_query, grad_keys, grad_values)
```

```python
import functools

import jax
import jax.numpy as jnp
from jax import lax
from jax.experimental import pallas as pl
from jax.experimental.pallas import tpu as pltpu
from jax.sharding import PartitionSpec as P

HD = 128
KVH = 8
GROUP = 5
BLK = 128
TOPK = 3
LANES = 128
CHUNKS = (32, 32, 32, 32)
LOG2E = 1.4426950408889634
SCALE = HD ** (-0.5)
MESH = pl.DeviceIdType.MESH
NT = (((1,), (1,)), ((), ()))
TN = (((0,), (0,)), ((), ()))
NN = (((1,), (0,)), ((), ()))


def dot(a, b, dims):
    return lax.dot_general(a, b, dims, preferred_element_type=jnp.float32)


def kernel(n, bulk, local_blocks, *refs):
    nc = len(CHUNKS)
    starts = [sum(CHUNKS[:c]) for c in range(nc)]
    items = local_blocks * KVH
    rows_q = GROUP * BLK
    refs = list(refs)

    def take(count):
        out = refs[:count]
        del refs[:count]
        return out

    q_hbm, g_hbm, o_hbm, k_hbm, v_hbm, lse_ref, comb_v, comb_s, sel_s = take(9)
    gq_hbm, gk_hbm, gv_hbm = take(3)
    q_s, g_s, o_s, kv_s, dq_s, own_s, delta_s, part_s, run_s, gq_s, gk_s, gv_s = take(12)
    reqs, tab_v, tab_s = take(3)
    out_c = take(nc)
    inf_c = take(nc)
    inb_c = take(nc)
    load_sem, misc_sem, send_sem, req_send, req_recv, recv_sem = take(6)

    me = lax.axis_index("ctx") * bulk + lax.axis_index("bulk")

    def place(peer):
        return (peer // bulk, peer % bulk)

    barrier = pltpu.get_barrier_semaphore()

    def greet(step, _):
        peer = (me + step) % n
        pl.semaphore_signal(barrier, inc=1, device_id=place(peer), device_id_type=MESH)
        return _

    lax.fori_loop(1, n, greet, 0)

    def load_heads(index, _):
        b = index // (KVH * GROUP)
        i = index % (KVH * GROUP)
        src = (pl.ds(pl.multiple_of(b * BLK, BLK), BLK), pl.ds(pl.multiple_of(i * HD, HD), HD))
        at = pl.ds(pl.multiple_of((i % GROUP) * BLK, BLK), BLK)
        item = b * KVH + i // GROUP
        pltpu.make_async_copy(g_hbm.at[src], g_s.at[item, at], load_sem.at[0]).start()
        pltpu.make_async_copy(o_hbm.at[src], o_s.at[item, at], load_sem.at[1]).start()
        pltpu.make_async_copy(q_hbm.at[src], q_s.at[item, at], load_sem.at[2]).start()
        return _

    def load_kv(index, _):
        b = index // KVH
        h = index % KVH
        src = (pl.ds(pl.multiple_of(b * BLK, BLK), BLK), pl.ds(pl.multiple_of(h * HD, HD), HD))
        pltpu.make_async_copy(k_hbm.at[src], kv_s.at[index, pl.ds(0, BLK)], load_sem.at[3]).start()
        pltpu.make_async_copy(v_hbm.at[src], kv_s.at[index, pl.ds(BLK, BLK)], load_sem.at[3]).start()
        return _

    lax.fori_loop(0, items, load_kv, 0)
    lax.fori_loop(0, items * GROUP, load_heads, 0)
    pl.semaphore_wait(barrier, n - 1)

    def req_copy(peer, row):
        at = pl.ds(pl.multiple_of(row * 8, 8), 8)
        return pltpu.make_async_remote_copy(
            src_ref=comb_v,
            dst_ref=reqs.at[at],
            send_sem=req_send.at[peer],
            recv_sem=req_recv.at[row],
            device_id=place(peer),
            device_id_type=MESH,
        )

    def send_req(peer, _):
        req_copy(peer, me).start()
        return _

    lax.fori_loop(0, me, send_req, 0)

    pltpu.make_async_copy(g_s, g_s, load_sem.at[0]).wait()
    pltpu.make_async_copy(o_s, o_s, load_sem.at[1]).wait()
    lane = lax.broadcasted_iota(jnp.int32, (BLK, LANES), 1)
    row = lax.broadcasted_iota(jnp.int32, (BLK, LANES), 0)
    for b in range(local_blocks):

        def one_delta(i, acc):
            item = b * KVH + i // GROUP
            at = pl.ds(pl.multiple_of((i % GROUP) * BLK, BLK), BLK)
            prod = g_s[item, at, :].astype(jnp.float32) * o_s[item, at, :].astype(jnp.float32)
            return jnp.where(lane == i, jnp.sum(prod, axis=1, keepdims=True), acc)

        acc = lax.fori_loop(0, KVH * GROUP, one_delta, jnp.zeros((BLK, LANES), jnp.float32))
        delta_s[b] = acc.T

    def wait_req(peer, _):
        req_copy(peer, peer).wait_recv()
        return _

    lax.fori_loop(me + 1, n, wait_req, 0)

    codes = reqs[pl.ds(0, n, 8), :]
    lane_n = lax.broadcasted_iota(jnp.int32, (n, LANES), 1)
    row_n = lax.broadcasted_iota(jnp.int32, (n, LANES), 0)
    code_col = jnp.sum(jnp.where((lane_n == me) & (row_n > me), codes, 0), axis=1, keepdims=True)
    code_col = jnp.where(row_n[:, :1] > me, code_col, -1)
    item_col = jnp.where(code_col >= 0, code_col % items, items)
    item_full = jnp.broadcast_to(item_col, (n, LANES))
    key_full = item_full * LANES + row_n
    diag = row_n == lane_n
    item_row = jnp.sum(jnp.where(diag, item_full, 0), axis=0, keepdims=True)
    key_row = jnp.sum(jnp.where(diag, key_full, 0), axis=0, keepdims=True)
    key_row = jnp.where(lane_n[:1] < n, key_row, LANES * LANES)
    rank_col = jnp.sum(jnp.where(key_row < key_full, 1, 0), axis=1, keepdims=True)
    order_row = jnp.sum(jnp.where(rank_col == lane_n, row_n, 0), axis=0, keepdims=True)
    upto_row = jnp.sum(jnp.where(item_full <= lane_n, 1, 0), axis=0, keepdims=True)
    below_row = jnp.sum(jnp.where(item_full < lane_n, 1, 0), axis=0, keepdims=True)
    sorted_row = jnp.sum(jnp.where(rank_col == lane_n, item_full, 0), axis=0, keepdims=True)
    tab_v[0:1, :] = jnp.minimum(item_row, items - 1)
    tab_v[1:2, :] = order_row
    tab_v[2:3, :] = jnp.maximum(upto_row - 1, 0)
    tab_v[3:4, :] = jnp.where(upto_row > below_row, 1, 0)
    tab_v[4:5, :] = sorted_row
    tab_copy = pltpu.make_async_copy(tab_v, tab_s, misc_sem.at[0])
    tab_copy.start()
    pltpu.make_async_copy(kv_s, kv_s, load_sem.at[3]).wait()
    tab_copy.wait()

    def data_copy(c, peer, source, box):
        return pltpu.make_async_remote_copy(
            src_ref=out_c[c].at[peer],
            dst_ref=box[c].at[source],
            send_sem=send_sem.at[c],
            recv_sem=recv_sem.at[c, source],
            device_id=place(peer),
            device_id_type=MESH,
        )

    stride = 37 if n == 128 else 1

    def stage_keys(c):
        size, at = CHUNKS[c], starts[c]

        def one(peer, _):
            want = tab_s[0, peer]
            out_c[c][peer, 0:size, :] = kv_s[want, at : at + size, :]
            out_c[c][peer, size : 2 * size, :] = kv_s[want, BLK + at : BLK + at + size, :]
            return _

        lax.fori_loop(me + 1, n, one, 0)

    def send_keys(c):
        def one(step, _):
            peer = (me + step * stride) % n

            @pl.when(peer > me)
            def go():
                data_copy(c, peer, me, inf_c).start()

            return _

        lax.fori_loop(1, n, one, 0)

    def stage_grads(c):
        def one(peer, _):
            slot = jnp.maximum(comb_s[peer], 0) // items
            out_c[c][peer] = part_s[slot, 0 : 2 * CHUNKS[c], :]
            return _

        lax.fori_loop(0, me, one, 0)

    def send_grads(c):
        def one(step, _):
            peer = (me + n - (step * stride) % n) % n

            @pl.when(peer < me)
            def go():
                data_copy(c, peer, me, inb_c).start()

            return _

        lax.fori_loop(1, n, one, 0)

    def wait_keys(c):
        def one(peer, _):
            data_copy(c, peer, peer, inf_c).wait_recv()
            return _

        lax.fori_loop(0, me, one, 0)

    def wait_grads(c):
        def one(peer, _):
            data_copy(c, peer, peer, inb_c).wait_recv()
            return _

        lax.fori_loop(me + 1, n, one, 0)

    def rows_of(item, box):
        b, h = item // KVH, item % KVH
        return jnp.concatenate([box[b, pl.ds(h * GROUP + g, 1), :] for g in range(GROUP)], axis=1)

    def attend(item, key_set, value_set, mask):
        queries, grads = q_s[item], g_s[item]
        scores = dot(key_set, queries, NT)
        probs32 = jnp.exp2(scores * (SCALE * LOG2E) - rows_of(item, lse_ref) * LOG2E)
        if mask is not None:
            probs32 = jnp.where(mask, probs32, 0.0)
        dprobs = dot(value_set, grads, NT)
        dscores = (probs32 * (dprobs - rows_of(item, delta_s))).astype(jnp.bfloat16)
        value_part = dot(probs32.astype(jnp.bfloat16), grads, NN)
        key_part = dot(dscores, queries, NN)
        return key_part, value_part, dot(key_set, dscores, TN)

    def own_block(item, _):
        key_at = lax.broadcasted_iota(jnp.int32, (BLK, rows_q), 0)
        query_at = lax.broadcasted_iota(jnp.int32, (BLK, rows_q), 1) % BLK
        key_part, value_part, query_part = attend(
            item, kv_s[item, 0:BLK, :], kv_s[item, BLK : 2 * BLK, :], key_at <= query_at
        )
        own_s[item, 0:BLK, :] = key_part
        own_s[item, BLK : 2 * BLK, :] = value_part
        dq_s[item] = query_part
        return _

    def chunk_grads(c):
        size = CHUNKS[c]

        def one(item, _):
            sets = []
            for s in range(TOPK):
                chosen = sel_s[item * TOPK + s]
                owner = jnp.where(chosen >= 0, chosen // local_blocks, n)
                sets.append(inf_c[c][owner])
            key_set = jnp.concatenate([x[:size] for x in sets], axis=0)
            value_set = jnp.concatenate([x[size:] for x in sets], axis=0)
            key_part, value_part, query_part = attend(item, key_set, value_set, None)
            for s in range(TOPK):
                at = slice(s * size, (s + 1) * size)
                part_s[item * TOPK + s, 0:size, :] = key_part[at].astype(jnp.bfloat16)
                part_s[item * TOPK + s, size : 2 * size, :] = value_part[at].astype(jnp.bfloat16)
            dq_s[item] += query_part
            return _

        lax.fori_loop(0, items, one, 0)

    def fold(c):
        size, at = CHUNKS[c], starts[c]

        def scan(k, acc):
            source = tab_s[1, k]
            fresh = (tab_s[4, k] != tab_s[4, jnp.maximum(k - 1, 0)]) | (k == 0)
            keep = jnp.where(fresh, 0.0, 1.0)
            acc = acc * keep + inb_c[c][source].astype(jnp.float32)
            run_s[k, 0 : 2 * size, :] = acc
            return acc

        lax.fori_loop(0, n - 1 - me, scan, jnp.zeros((2 * size, HD), jnp.float32))

        def finish(item, _):
            last = jnp.where(tab_s[3, item] > 0, tab_s[2, item], n)
            total = run_s[last, 0 : 2 * size, :]
            b, h = item // KVH, item % KVH
            rows = pl.ds(pl.multiple_of(b * BLK + at, 16), size)
            cols = pl.ds(pl.multiple_of(h * HD, HD), HD)
            key_sum = own_s[item, at : at + size, :] + total[:size]
            value_sum = own_s[item, BLK + at : BLK + at + size, :] + total[size:]
            gk_s[rows, cols] = (key_sum * SCALE).astype(jnp.bfloat16)
            gv_s[rows, cols] = value_sum.astype(jnp.bfloat16)
            return _

        lax.fori_loop(0, items, finish, 0)

    for c in range(nc):
        inf_c[c][n] = jnp.zeros((2 * CHUNKS[c], HD), jnp.bfloat16)
    run_s[n] = jnp.zeros(run_s.shape[1:], jnp.float32)

    stage_keys(0)
    if nc > 1:
        stage_keys(1)
    send_keys(0)
    if nc > 1:
        send_keys(1)
    for c in range(2, nc):
        stage_keys(c)
    pltpu.make_async_copy(q_s, q_s, load_sem.at[2]).wait()
    lax.fori_loop(0, items, own_block, 0)

    for c in range(nc):
        wait_keys(c)
        chunk_grads(c)
        stage_grads(c)
        send_grads(c)
        if c + 2 < nc:
            send_keys(c + 2)

    def finish_query(index, _):
        b = index // (KVH * GROUP)
        i = index % (KVH * GROUP)
        item = b * KVH + i // GROUP
        cols = pl.ds(pl.multiple_of((i % GROUP) * BLK, BLK), BLK)
        rows = pl.ds(pl.multiple_of(b * BLK, BLK), BLK)
        part = dq_s[item, :, cols].T * SCALE
        gq_s[rows, pl.ds(pl.multiple_of(i * HD, HD), HD)] = part.astype(jnp.bfloat16)
        return _

    lax.fori_loop(0, items * GROUP, finish_query, 0)
    out_q = pltpu.make_async_copy(gq_s, gq_hbm, misc_sem.at[1])
    out_q.start()

    for c in range(nc):
        wait_grads(c)
        fold(c)
    out_k = pltpu.make_async_copy(gk_s, gk_hbm, misc_sem.at[2])
    out_v = pltpu.make_async_copy(gv_s, gv_hbm, misc_sem.at[3])
    out_k.start()
    out_v.start()

    def wait_req_sent(peer, _):
        req_copy(peer, me).wait_send()
        return _

    lax.fori_loop(0, me, wait_req_sent, 0)
    for c in range(nc):
        sent = out_c[c].at[pl.ds(0, n - 1)]
        pltpu.make_async_copy(sent, sent, send_sem.at[c]).wait()
    out_q.wait()
    out_k.wait()
    out_v.wait()


def shards(query, keys, values, output, grad_out, logsumexp, selected):
    bulk = lax.axis_size("bulk")
    n = lax.axis_size("ctx") * bulk
    tokens = query.shape[0]
    local_blocks = tokens // BLK
    items = local_blocks * KVH
    per_device = items * TOPK
    chosen = selected.reshape(per_device)
    slots = jnp.arange(per_device, dtype=jnp.int32)
    code = slots * items + chosen % local_blocks * KVH + slots // TOPK % KVH
    owners = jnp.where(chosen >= 0, chosen // local_blocks, -1)
    matches = owners[:, None] == jnp.arange(LANES, dtype=jnp.int32)[None, :]
    comb = jnp.max(jnp.where(matches, code[:, None], -1), axis=0)
    comb_tile = jnp.broadcast_to(comb[None, :], (8, LANES))
    lse = jnp.transpose(logsumexp.reshape(local_blocks, BLK, KVH * GROUP), (0, 2, 1))
    bf16, f32, i32 = jnp.bfloat16, jnp.float32, jnp.int32
    nc = len(CHUNKS)
    widest = max(CHUNKS)
    any_spec = pl.BlockSpec(memory_space=pl.ANY)
    vmem = pl.BlockSpec(memory_space=pltpu.VMEM)
    smem = pl.BlockSpec(memory_space=pltpu.SMEM)
    scratch = [
        pltpu.VMEM((items, GROUP * BLK, HD), bf16),
        pltpu.VMEM((items, GROUP * BLK, HD), bf16),
        pltpu.VMEM((items, GROUP * BLK, HD), bf16),
        pltpu.VMEM((items, 2 * BLK, HD), bf16),
        pltpu.VMEM((items, HD, GROUP * BLK), f32),
        pltpu.VMEM((items, 2 * BLK, HD), f32),
        pltpu.VMEM((local_blocks, LANES, BLK), f32),
        pltpu.VMEM((per_device, 2 * widest, HD), bf16),
        pltpu.VMEM((n + 1, 2 * widest, HD), f32),
        pltpu.VMEM(query.shape, bf16),
        pltpu.VMEM(keys.shape, bf16),
        pltpu.VMEM(values.shape, bf16),
        pltpu.VMEM((8 * n, LANES), i32),
        pltpu.VMEM((8, LANES), i32),
        pltpu.SMEM((8, LANES), i32),
        *[pltpu.VMEM((n, 2 * size, HD), bf16) for size in CHUNKS],
        *[pltpu.VMEM((n + 1, 2 * size, HD), bf16) for size in CHUNKS],
        *[pltpu.VMEM((n, 2 * size, HD), bf16) for size in CHUNKS],
        pltpu.SemaphoreType.DMA((4,)),
        pltpu.SemaphoreType.DMA((4,)),
        pltpu.SemaphoreType.DMA((nc,)),
        pltpu.SemaphoreType.DMA((n,)),
        pltpu.SemaphoreType.DMA((n,)),
        pltpu.SemaphoreType.DMA((nc, n)),
    ]
    return pl.pallas_call(
        functools.partial(kernel, n, bulk, local_blocks),
        out_shape=(
            jax.ShapeDtypeStruct(query.shape, bf16),
            jax.ShapeDtypeStruct(keys.shape, bf16),
            jax.ShapeDtypeStruct(values.shape, bf16),
        ),
        in_specs=[any_spec] * 5 + [vmem, vmem, smem, smem],
        out_specs=(any_spec,) * 3,
        scratch_shapes=scratch,
        compiler_params=pltpu.CompilerParams(
            collective_id=0, has_side_effects=True, vmem_limit_bytes=63_000_000
        ),
        name="block_sparse_backward",
    )(query, grad_out, output, keys, values, lse, comb_tile, comb, chosen)


def solution(mesh):
    rows = P(("ctx", "bulk"), None)
    in_specs = (rows,) * 6 + (P(("ctx", "bulk"), None, None),)
    return jax.shard_map(
        shards, mesh=mesh, in_specs=in_specs, out_specs=(rows,) * 3, check_vma=False
    )
```

```python
import functools

import jax
import jax.numpy as jnp
from jax import lax
from jax.experimental import pallas as pl
from jax.experimental.pallas import tpu as pltpu
from jax.sharding import PartitionSpec as P

HD = 128
KVH = 8
GROUP = 5
BLK = 128
TOPK = 3
LANES = 128
CHUNKS = (16,) * 8
AHEAD = 2
STRIDE = 37
LOG2E = 1.4426950408889634
SCALE = HD ** (-0.5)
MESH = pl.DeviceIdType.MESH
NT = (((1,), (1,)), ((), ()))
TN = (((0,), (0,)), ((), ()))
NN = (((1,), (0,)), ((), ()))


def dot(a, b, dims):
    return lax.dot_general(a, b, dims, preferred_element_type=jnp.float32)


def kernel(n, bulk, local_blocks, *refs):
    nc = len(CHUNKS)
    starts = [sum(CHUNKS[:c]) for c in range(nc)]
    items = local_blocks * KVH
    rows_q = GROUP * BLK
    refs = list(refs)

    def take(count):
        out = refs[:count]
        del refs[:count]
        return out

    q_hbm, g_hbm, o_hbm, k_hbm, v_hbm, lse_ref, comb_s, sel_s = take(8)
    gq_hbm, gk_hbm, gv_hbm = take(3)
    q_s, g_s, o_s, kv_s, dq_s, own_s, delta_s, part_s, run_s, gq_s, gk_s, gv_s = take(12)
    reqs_s, reqs_v, tab_v, tab_s = take(4)
    out_c = take(nc)
    inf_c = take(nc)
    inb_c = take(nc)
    load_sem, misc_sem, send_sem, req_send, req_recv, recv_sem = take(6)

    me = lax.axis_index("ctx") * bulk + lax.axis_index("bulk")

    def place(peer):
        return (peer // bulk, peer % bulk)

    barrier = pltpu.get_barrier_semaphore()

    def greet(step, _):
        peer = (me + step) % n
        pl.semaphore_signal(barrier, inc=1, device_id=place(peer), device_id_type=MESH)
        return _

    lax.fori_loop(1, n, greet, 0)

    def load_heads(index, _):
        b = index // (KVH * GROUP)
        i = index % (KVH * GROUP)
        src = (pl.ds(pl.multiple_of(b * BLK, BLK), BLK), pl.ds(pl.multiple_of(i * HD, HD), HD))
        at = pl.ds(pl.multiple_of((i % GROUP) * BLK, BLK), BLK)
        item = b * KVH + i // GROUP
        pltpu.make_async_copy(g_hbm.at[src], g_s.at[item, at], load_sem.at[0]).start()
        pltpu.make_async_copy(o_hbm.at[src], o_s.at[item, at], load_sem.at[1]).start()
        pltpu.make_async_copy(q_hbm.at[src], q_s.at[item, at], load_sem.at[2]).start()
        return _

    def load_kv(index, _):
        b = index // KVH
        h = index % KVH
        src = (pl.ds(pl.multiple_of(b * BLK, BLK), BLK), pl.ds(pl.multiple_of(h * HD, HD), HD))
        pltpu.make_async_copy(k_hbm.at[src], kv_s.at[index, pl.ds(0, BLK)], load_sem.at[3]).start()
        pltpu.make_async_copy(v_hbm.at[src], kv_s.at[index, pl.ds(BLK, BLK)], load_sem.at[3]).start()
        return _

    lax.fori_loop(0, items, load_kv, 0)
    lax.fori_loop(0, items * GROUP, load_heads, 0)
    pl.semaphore_wait(barrier, n - 1)

    def req_copy(peer, row):
        return pltpu.make_async_remote_copy(
            src_ref=comb_s,
            dst_ref=reqs_s.at[pl.ds(row, 1)],
            send_sem=req_send.at[peer],
            recv_sem=req_recv.at[row],
            device_id=place(peer),
            device_id_type=MESH,
        )

    def send_req(peer, _):
        req_copy(peer, me).start()
        return _

    lax.fori_loop(0, me, send_req, 0)

    pltpu.make_async_copy(g_s, g_s, load_sem.at[0]).wait()
    pltpu.make_async_copy(o_s, o_s, load_sem.at[1]).wait()
    lane = lax.broadcasted_iota(jnp.int32, (BLK, LANES), 1)
    row = lax.broadcasted_iota(jnp.int32, (BLK, LANES), 0)
    for b in range(local_blocks):

        def one_delta(i, acc):
            item = b * KVH + i // GROUP
            at = pl.ds(pl.multiple_of((i % GROUP) * BLK, BLK), BLK)
            prod = g_s[item, at, :].astype(jnp.float32) * o_s[item, at, :].astype(jnp.float32)
            return jnp.where(lane == i, jnp.sum(prod, axis=1, keepdims=True), acc)

        acc = lax.fori_loop(0, KVH * GROUP, one_delta, jnp.zeros((BLK, LANES), jnp.float32))
        delta_s[b] = acc.T

    def wait_req(peer, _):
        req_copy(peer, peer).wait_recv()
        return _

    lax.fori_loop(me + 1, n, wait_req, 0)

    pltpu.make_async_copy(kv_s, kv_s, load_sem.at[3]).wait()

    def data_copy(c, peer, source, box):
        return pltpu.make_async_remote_copy(
            src_ref=out_c[c].at[peer],
            dst_ref=box[c].at[source],
            send_sem=send_sem.at[c],
            recv_sem=recv_sem.at[c, source],
            device_id=place(peer),
            device_id_type=MESH,
        )

    stride = STRIDE if n == 128 else 1

    def stage_keys(c):
        size, at = CHUNKS[c], starts[c]

        def one(peer, _):
            want = lax.rem(jnp.maximum(reqs_s[peer, me], 0), items)
            out_c[c][peer, 0:size, :] = kv_s[want, at : at + size, :]
            out_c[c][peer, size : 2 * size, :] = kv_s[want, BLK + at : BLK + at + size, :]
            return _

        lax.fori_loop(me + 1, n, one, 0)

    def send(keys_c, grads_c):
        def one(step, _):
            peer = (me + step * stride) % n
            if keys_c is not None:

                @pl.when(peer > me)
                def go_keys():
                    data_copy(keys_c, peer, me, inf_c).start()

            if grads_c is not None:

                @pl.when(peer < me)
                def go_grads():
                    data_copy(grads_c, peer, me, inb_c).start()

            return _

        lax.fori_loop(1, n, one, 0)

    def stage_grads(c):
        def one(peer, _):
            slot = lax.div(jnp.maximum(comb_s[0, peer], 0), items)
            out_c[c][peer] = part_s[slot, 0 : 2 * CHUNKS[c], :]
            return _

        lax.fori_loop(0, me, one, 0)

    def wait_keys(c):
        def one(peer, _):
            data_copy(c, peer, peer, inf_c).wait_recv()
            return _

        lax.fori_loop(0, me, one, 0)

    def wait_grads(c):
        def one(peer, _):
            data_copy(c, peer, peer, inb_c).wait_recv()
            return _

        lax.fori_loop(me + 1, n, one, 0)

    def rows_of(item, box):
        b, h = item // KVH, item % KVH
        return jnp.concatenate([box[b, pl.ds(h * GROUP + g, 1), :] for g in range(GROUP)], axis=1)

    def attend(item, key_set, value_set, mask):
        queries, grads = q_s[item], g_s[item]
        scores = dot(key_set, queries, NT)
        probs32 = jnp.exp2(scores * (SCALE * LOG2E) - rows_of(item, lse_ref) * LOG2E)
        if mask is not None:
            probs32 = jnp.where(mask, probs32, 0.0)
        dprobs = dot(value_set, grads, NT)
        dscores = (probs32 * (dprobs - rows_of(item, delta_s))).astype(jnp.bfloat16)
        value_part = dot(probs32.astype(jnp.bfloat16), grads, NN)
        key_part = dot(dscores, queries, NN)
        return key_part, value_part, dot(key_set, dscores, TN)

    def own_block(item, _):
        key_at = lax.broadcasted_iota(jnp.int32, (BLK, rows_q), 0)
        query_at = lax.broadcasted_iota(jnp.int32, (BLK, rows_q), 1) % BLK
        key_part, value_part, query_part = attend(
            item, kv_s[item, 0:BLK, :], kv_s[item, BLK : 2 * BLK, :], key_at <= query_at
        )
        own_s[item, 0:BLK, :] = key_part
        own_s[item, BLK : 2 * BLK, :] = value_part
        dq_s[item] = query_part
        return _

    def chunk_grads(c):
        size = CHUNKS[c]

        def one(item, _):
            sets = []
            for s in range(TOPK):
                chosen = sel_s[item * TOPK + s]
                owner = jnp.where(chosen >= 0, chosen // local_blocks, n)
                sets.append(inf_c[c][owner])
            key_set = jnp.concatenate([x[:size] for x in sets], axis=0)
            value_set = jnp.concatenate([x[size:] for x in sets], axis=0)
            key_part, value_part, query_part = attend(item, key_set, value_set, None)
            for s in range(TOPK):
                at = slice(s * size, (s + 1) * size)
                part_s[item * TOPK + s, 0:size, :] = key_part[at].astype(jnp.bfloat16)
                part_s[item * TOPK + s, size : 2 * size, :] = value_part[at].astype(jnp.bfloat16)
            dq_s[item] += query_part
            return _

        lax.fori_loop(0, items, one, 0)

    def fold(c):
        size, at = CHUNKS[c], starts[c]

        def scan(k, acc):
            source = tab_s[1, k]
            fresh = (tab_s[4, k] != tab_s[4, jnp.maximum(k - 1, 0)]) | (k == 0)
            keep = jnp.where(fresh, 0.0, 1.0)
            acc = acc * keep + inb_c[c][source].astype(jnp.float32)
            run_s[k, 0 : 2 * size, :] = acc
            return acc

        lax.fori_loop(0, n - 1 - me, scan, jnp.zeros((2 * size, HD), jnp.float32))

        def finish(item, _):
            last = jnp.where(tab_s[3, item] > 0, tab_s[2, item], n)
            total = run_s[last, 0 : 2 * size, :]
            b, h = item // KVH, item % KVH
            rows = pl.ds(pl.multiple_of(b * BLK + at, 16), size)
            cols = pl.ds(pl.multiple_of(h * HD, HD), HD)
            key_sum = own_s[item, at : at + size, :] + total[:size]
            value_sum = own_s[item, BLK + at : BLK + at + size, :] + total[size:]
            gk_s[rows, cols] = (key_sum * SCALE).astype(jnp.bfloat16)
            gv_s[rows, cols] = value_sum.astype(jnp.bfloat16)
            return _

        lax.fori_loop(0, items, finish, 0)

    for c in range(AHEAD):
        stage_keys(c)
        send(c, None)
    req_vector = pltpu.make_async_copy(reqs_s, reqs_v, misc_sem.at[4])
    req_vector.start()
    for c in range(nc):
        inf_c[c][n] = jnp.zeros((2 * CHUNKS[c], HD), jnp.bfloat16)
    run_s[n] = jnp.zeros(run_s.shape[1:], jnp.float32)
    for c in range(AHEAD, nc):
        stage_keys(c)
    req_vector.wait()
    lane_n = lax.broadcasted_iota(jnp.int32, (n, LANES), 1)
    row_n = lax.broadcasted_iota(jnp.int32, (n, LANES), 0)
    code_col = jnp.sum(jnp.where((lane_n == me) & (row_n > me), reqs_v[...], 0), axis=1, keepdims=True)
    code_col = jnp.where(row_n[:, :1] > me, code_col, -1)
    item_col = jnp.where(code_col >= 0, code_col % items, items)
    item_full = jnp.broadcast_to(item_col, (n, LANES))
    key_full = item_full * LANES + row_n
    diag = row_n == lane_n
    key_row = jnp.sum(jnp.where(diag, key_full, 0), axis=0, keepdims=True)
    key_row = jnp.where(lane_n[:1] < n, key_row, LANES * LANES)
    rank_col = jnp.sum(jnp.where(key_row < key_full, 1, 0), axis=1, keepdims=True)
    order_row = jnp.sum(jnp.where(rank_col == lane_n, row_n, 0), axis=0, keepdims=True)
    upto_row = jnp.sum(jnp.where(item_full <= lane_n, 1, 0), axis=0, keepdims=True)
    below_row = jnp.sum(jnp.where(item_full < lane_n, 1, 0), axis=0, keepdims=True)
    sorted_row = jnp.sum(jnp.where(rank_col == lane_n, item_full, 0), axis=0, keepdims=True)
    tab_v[1:2, :] = order_row
    tab_v[2:3, :] = jnp.maximum(upto_row - 1, 0)
    tab_v[3:4, :] = jnp.where(upto_row > below_row, 1, 0)
    tab_v[4:5, :] = sorted_row
    tab_copy = pltpu.make_async_copy(tab_v, tab_s, misc_sem.at[0])
    tab_copy.start()

    pltpu.make_async_copy(q_s, q_s, load_sem.at[2]).wait()
    lax.fori_loop(0, items, own_block, 0)

    for c in range(nc):
        wait_keys(c)
        chunk_grads(c)
        stage_grads(c)
        send(c + AHEAD if c + AHEAD < nc else None, c)
    tab_copy.wait()

    def finish_query(index, _):
        b = index // (KVH * GROUP)
        i = index % (KVH * GROUP)
        item = b * KVH + i // GROUP
        cols = pl.ds(pl.multiple_of((i % GROUP) * BLK, BLK), BLK)
        rows = pl.ds(pl.multiple_of(b * BLK, BLK), BLK)
        part = dq_s[item, :, cols].T * SCALE
        gq_s[rows, pl.ds(pl.multiple_of(i * HD, HD), HD)] = part.astype(jnp.bfloat16)
        return _

    lax.fori_loop(0, items * GROUP, finish_query, 0)
    out_q = pltpu.make_async_copy(gq_s, gq_hbm, misc_sem.at[1])
    out_q.start()

    for c in range(nc):
        wait_grads(c)
        fold(c)
    out_k = pltpu.make_async_copy(gk_s, gk_hbm, misc_sem.at[2])
    out_v = pltpu.make_async_copy(gv_s, gv_hbm, misc_sem.at[3])
    out_k.start()
    out_v.start()

    def wait_req_sent(peer, _):
        req_copy(peer, me).wait_send()
        return _

    lax.fori_loop(0, me, wait_req_sent, 0)
    for c in range(nc):
        sent = out_c[c].at[pl.ds(0, n - 1)]
        pltpu.make_async_copy(sent, sent, send_sem.at[c]).wait()
    out_q.wait()
    out_k.wait()
    out_v.wait()


def shards(query, keys, values, output, grad_out, logsumexp, selected):
    bulk = lax.axis_size("bulk")
    n = lax.axis_size("ctx") * bulk
    tokens = query.shape[0]
    local_blocks = tokens // BLK
    items = local_blocks * KVH
    per_device = items * TOPK
    chosen = selected.reshape(per_device)
    slots = jnp.arange(per_device, dtype=jnp.int32)
    code = slots * items + chosen % local_blocks * KVH + slots // TOPK % KVH
    owners = jnp.where(chosen >= 0, chosen // local_blocks, -1)
    matches = owners[:, None] == jnp.arange(LANES, dtype=jnp.int32)[None, :]
    comb = jnp.max(jnp.where(matches, code[:, None], -1), axis=0)
    lse = jnp.transpose(logsumexp.reshape(local_blocks, BLK, KVH * GROUP), (0, 2, 1))
    bf16, f32, i32 = jnp.bfloat16, jnp.float32, jnp.int32
    nc = len(CHUNKS)
    widest = max(CHUNKS)
    any_spec = pl.BlockSpec(memory_space=pl.ANY)
    vmem = pl.BlockSpec(memory_space=pltpu.VMEM)
    smem = pl.BlockSpec(memory_space=pltpu.SMEM)
    scratch = [
        pltpu.VMEM((items, GROUP * BLK, HD), bf16),
        pltpu.VMEM((items, GROUP * BLK, HD), bf16),
        pltpu.VMEM((items, GROUP * BLK, HD), bf16),
        pltpu.VMEM((items, 2 * BLK, HD), bf16),
        pltpu.VMEM((items, HD, GROUP * BLK), f32),
        pltpu.VMEM((items, 2 * BLK, HD), f32),
        pltpu.VMEM((local_blocks, LANES, BLK), f32),
        pltpu.VMEM((per_device, 2 * widest, HD), bf16),
        pltpu.VMEM((n + 1, 2 * widest, HD), f32),
        pltpu.VMEM(query.shape, bf16),
        pltpu.VMEM(keys.shape, bf16),
        pltpu.VMEM(values.shape, bf16),
        pltpu.SMEM((n, LANES), i32),
        pltpu.VMEM((n, LANES), i32),
        pltpu.VMEM((8, LANES), i32),
        pltpu.SMEM((8, LANES), i32),
        *[pltpu.VMEM((n, 2 * size, HD), bf16) for size in CHUNKS],
        *[pltpu.VMEM((n + 1, 2 * size, HD), bf16) for size in CHUNKS],
        *[pltpu.VMEM((n, 2 * size, HD), bf16) for size in CHUNKS],
        pltpu.SemaphoreType.DMA((4,)),
        pltpu.SemaphoreType.DMA((5,)),
        pltpu.SemaphoreType.DMA((nc,)),
        pltpu.SemaphoreType.DMA((n,)),
        pltpu.SemaphoreType.DMA((n,)),
        pltpu.SemaphoreType.DMA((nc, n)),
    ]
    return pl.pallas_call(
        functools.partial(kernel, n, bulk, local_blocks),
        out_shape=(
            jax.ShapeDtypeStruct(query.shape, bf16),
            jax.ShapeDtypeStruct(keys.shape, bf16),
            jax.ShapeDtypeStruct(values.shape, bf16),
        ),
        in_specs=[any_spec] * 5 + [vmem, smem, smem],
        out_specs=(any_spec,) * 3,
        scratch_shapes=scratch,
        compiler_params=pltpu.CompilerParams(
            collective_id=0, has_side_effects=True, vmem_limit_bytes=63_000_000
        ),
        name="block_sparse_backward",
    )(query, grad_out, output, keys, values, lse, comb[None, :], chosen)


def solution(mesh):
    rows = P(("ctx", "bulk"), None)
    in_specs = (rows,) * 6 + (P(("ctx", "bulk"), None, None),)
    return jax.shard_map(
        shards, mesh=mesh, in_specs=in_specs, out_specs=(rows,) * 3, check_vma=False
    )
```

```python
import functools

import jax
import jax.numpy as jnp
from jax import lax
from jax.experimental import pallas as pl
from jax.experimental.pallas import tpu as pltpu
from jax.sharding import PartitionSpec as P

HD = 128
KVH = 8
GROUP = 5
BLK = 128
TOPK = 3
LANES = 128
CHUNKS = (16,) * 8
AHEAD = 2
STRIDE = 91
UNROLL = 4
LOG2E = 1.4426950408889634
SCALE = HD ** (-0.5)
MESH = pl.DeviceIdType.MESH
NT = (((1,), (1,)), ((), ()))
TN = (((0,), (0,)), ((), ()))
NN = (((1,), (0,)), ((), ()))


def dot(a, b, dims):
    return lax.dot_general(a, b, dims, preferred_element_type=jnp.float32)


def kernel(n, bulk, local_blocks, *refs):
    nc = len(CHUNKS)
    starts = [sum(CHUNKS[:c]) for c in range(nc)]
    items = local_blocks * KVH
    rows_q = GROUP * BLK
    refs = list(refs)

    def take(count):
        out = refs[:count]
        del refs[:count]
        return out

    q_hbm, g_hbm, o_hbm, k_hbm, v_hbm, lse_ref, comb_s, sel_s = take(8)
    gq_hbm, gk_hbm, gv_hbm = take(3)
    q_s, g_s, o_s, kv_s, dq_s, own_s, delta_s, part_s, run_s, gq_s, gk_s, gv_s = take(12)
    reqs_s, reqs_v, tab_v, tab_s = take(4)
    outf_c = take(nc)
    outb_c = take(nc)
    inf_c = take(nc)
    inb_c = take(nc)
    load_sem, misc_sem, send_sem, req_send, req_recv, recv_sem = take(6)

    me = lax.axis_index("ctx") * bulk + lax.axis_index("bulk")

    def place(peer):
        return (lax.div(peer, bulk), lax.rem(peer, bulk))

    barrier = pltpu.get_barrier_semaphore()

    def greet(step, _):
        peer = lax.rem(me + step, n)
        pl.semaphore_signal(barrier, inc=1, device_id=place(peer), device_id_type=MESH)
        return _

    lax.fori_loop(1, n, greet, 0)

    def load_heads(index, _):
        b = index // (KVH * GROUP)
        i = index % (KVH * GROUP)
        src = (pl.ds(pl.multiple_of(b * BLK, BLK), BLK), pl.ds(pl.multiple_of(i * HD, HD), HD))
        at = pl.ds(pl.multiple_of((i % GROUP) * BLK, BLK), BLK)
        item = b * KVH + i // GROUP
        pltpu.make_async_copy(g_hbm.at[src], g_s.at[item, at], load_sem.at[0]).start()
        pltpu.make_async_copy(o_hbm.at[src], o_s.at[item, at], load_sem.at[1]).start()
        pltpu.make_async_copy(q_hbm.at[src], q_s.at[item, at], load_sem.at[2]).start()
        return _

    def load_kv(index, _):
        b = index // KVH
        h = index % KVH
        src = (pl.ds(pl.multiple_of(b * BLK, BLK), BLK), pl.ds(pl.multiple_of(h * HD, HD), HD))
        pltpu.make_async_copy(k_hbm.at[src], kv_s.at[index, pl.ds(0, BLK)], load_sem.at[3]).start()
        pltpu.make_async_copy(v_hbm.at[src], kv_s.at[index, pl.ds(BLK, BLK)], load_sem.at[3]).start()
        return _

    lax.fori_loop(0, items, load_kv, 0)
    lax.fori_loop(0, items * GROUP, load_heads, 0)
    pl.semaphore_wait(barrier, n - 1)

    def req_copy(peer, row):
        return pltpu.make_async_remote_copy(
            src_ref=comb_s,
            dst_ref=reqs_s.at[pl.ds(row, 1)],
            send_sem=req_send.at[peer],
            recv_sem=req_recv.at[row],
            device_id=place(peer),
            device_id_type=MESH,
        )

    def send_req(peer, _):
        req_copy(peer, me).start()
        return _

    lax.fori_loop(0, me, send_req, 0)

    pltpu.make_async_copy(g_s, g_s, load_sem.at[0]).wait()
    pltpu.make_async_copy(o_s, o_s, load_sem.at[1]).wait()
    lane = lax.broadcasted_iota(jnp.int32, (BLK, LANES), 1)
    row = lax.broadcasted_iota(jnp.int32, (BLK, LANES), 0)
    for b in range(local_blocks):

        def one_delta(i, acc):
            item = b * KVH + i // GROUP
            at = pl.ds(pl.multiple_of((i % GROUP) * BLK, BLK), BLK)
            prod = g_s[item, at, :].astype(jnp.float32) * o_s[item, at, :].astype(jnp.float32)
            return jnp.where(lane == i, jnp.sum(prod, axis=1, keepdims=True), acc)

        acc = lax.fori_loop(0, KVH * GROUP, one_delta, jnp.zeros((BLK, LANES), jnp.float32))
        delta_s[b] = acc.T

    def wait_req(peer, _):
        req_copy(peer, peer).wait_recv()
        return _

    lax.fori_loop(me + 1, n, wait_req, 0)

    pltpu.make_async_copy(kv_s, kv_s, load_sem.at[3]).wait()

    def data_copy(c, peer, source, out, box, turn=0):
        return pltpu.make_async_remote_copy(
            src_ref=out[c].at[peer],
            dst_ref=box[c].at[source],
            send_sem=send_sem.at[turn % 2, peer],
            recv_sem=recv_sem.at[c, source],
            device_id=place(peer),
            device_id_type=MESH,
        )

    stride = STRIDE if n == 128 else 1

    def stage_keys(c):
        size, at = CHUNKS[c], starts[c]

        def one(peer, _):
            want = lax.rem(jnp.maximum(reqs_s[peer, me], 0), items)
            outf_c[c][peer, 0:size, :] = kv_s[want, at : at + size, :]
            outf_c[c][peer, size : 2 * size, :] = kv_s[want, BLK + at : BLK + at + size, :]
            return _

        lax.fori_loop(0, n, one, 0, unroll=UNROLL)

    def wait_sent(turn):
        def keys_sent(peer, _):
            data_copy(turn, peer, me, outf_c, inf_c, turn).wait_send()
            return _

        def grads_sent(peer, _):
            data_copy(turn - AHEAD, peer, me, outb_c, inb_c, turn).wait_send()
            return _

        if 0 <= turn < nc:
            lax.fori_loop(me + 1, n, keys_sent, 0)
        if AHEAD <= turn:
            lax.fori_loop(0, me, grads_sent, 0)

    def send(turn):
        keys_c = turn if turn < nc else None
        grads_c = turn - AHEAD if turn >= AHEAD else None
        wait_sent(turn - 2)

        def one(step, _):
            peer = lax.rem(me + step * stride, n)
            if keys_c is not None:

                @pl.when(peer > me)
                def go_keys():
                    data_copy(keys_c, peer, me, outf_c, inf_c, turn).start()

            if grads_c is not None:

                @pl.when(peer < me)
                def go_grads():
                    data_copy(grads_c, peer, me, outb_c, inb_c, turn).start()

            return _

        lax.fori_loop(0, n, one, 0, unroll=UNROLL)

    def stage_grads(c):
        def one(peer, _):
            slot = lax.div(jnp.maximum(comb_s[0, peer], 0), items)
            outb_c[c][peer] = part_s[slot, 0 : 2 * CHUNKS[c], :]
            return _

        lax.fori_loop(0, n, one, 0, unroll=UNROLL)

    def wait_keys(c):
        def one(peer, _):
            data_copy(c, peer, peer, outf_c, inf_c).wait_recv()
            return _

        lax.fori_loop(0, me, one, 0)

    def wait_grads(c):
        def one(peer, _):
            data_copy(c, peer, peer, outb_c, inb_c).wait_recv()
            return _

        lax.fori_loop(me + 1, n, one, 0)

    def rows_of(item, box):
        b, h = item // KVH, item % KVH
        return jnp.concatenate([box[b, pl.ds(h * GROUP + g, 1), :] for g in range(GROUP)], axis=1)

    def attend(item, key_set, value_set, mask):
        queries, grads = q_s[item], g_s[item]
        scores = dot(key_set, queries, NT)
        probs32 = jnp.exp2(scores * (SCALE * LOG2E) - rows_of(item, lse_ref) * LOG2E)
        if mask is not None:
            probs32 = jnp.where(mask, probs32, 0.0)
        dprobs = dot(value_set, grads, NT)
        dscores = (probs32 * (dprobs - rows_of(item, delta_s))).astype(jnp.bfloat16)
        value_part = dot(probs32.astype(jnp.bfloat16), grads, NN)
        key_part = dot(dscores, queries, NN)
        return key_part, value_part, dot(key_set, dscores, TN)

    def own_block(item, _):
        key_at = lax.broadcasted_iota(jnp.int32, (BLK, rows_q), 0)
        query_at = lax.broadcasted_iota(jnp.int32, (BLK, rows_q), 1) % BLK
        key_part, value_part, query_part = attend(
            item, kv_s[item, 0:BLK, :], kv_s[item, BLK : 2 * BLK, :], key_at <= query_at
        )
        own_s[item, 0:BLK, :] = key_part
        own_s[item, BLK : 2 * BLK, :] = value_part
        dq_s[item] = query_part
        return _

    def chunk_grads(c):
        size = CHUNKS[c]

        def one(item, _):
            sets = []
            for s in range(TOPK):
                chosen = sel_s[item * TOPK + s]
                owner = jnp.where(chosen >= 0, chosen // local_blocks, n)
                sets.append(inf_c[c][owner])
            key_set = jnp.concatenate([x[:size] for x in sets], axis=0)
            value_set = jnp.concatenate([x[size:] for x in sets], axis=0)
            key_part, value_part, query_part = attend(item, key_set, value_set, None)
            for s in range(TOPK):
                at = slice(s * size, (s + 1) * size)
                part_s[item * TOPK + s, 0:size, :] = key_part[at].astype(jnp.bfloat16)
                part_s[item * TOPK + s, size : 2 * size, :] = value_part[at].astype(jnp.bfloat16)
            dq_s[item] += query_part
            return _

        lax.fori_loop(0, items, one, 0)

    def fold(c):
        size, at = CHUNKS[c], starts[c]

        def scan(k, acc):
            source = tab_s[1, k]
            acc = jnp.where(tab_s[4, k] > 0, 0.0, acc) + inb_c[c][source].astype(jnp.float32)
            run_s[k, 0 : 2 * size, :] = acc
            return acc

        lax.fori_loop(0, n, scan, jnp.zeros((2 * size, HD), jnp.float32), unroll=UNROLL)

        def finish(item, _):
            last = jnp.where(tab_s[3, item] > 0, tab_s[2, item], n)
            total = run_s[last, 0 : 2 * size, :]
            b, h = item // KVH, item % KVH
            rows = pl.ds(pl.multiple_of(b * BLK + at, 16), size)
            cols = pl.ds(pl.multiple_of(h * HD, HD), HD)
            key_sum = own_s[item, at : at + size, :] + total[:size]
            value_sum = own_s[item, BLK + at : BLK + at + size, :] + total[size:]
            gk_s[rows, cols] = (key_sum * SCALE).astype(jnp.bfloat16)
            gv_s[rows, cols] = value_sum.astype(jnp.bfloat16)
            return _

        lax.fori_loop(0, items, finish, 0, unroll=UNROLL)

    for c in range(AHEAD):
        stage_keys(c)
        send(c)
    req_vector = pltpu.make_async_copy(reqs_s, reqs_v, misc_sem.at[4])
    req_vector.start()
    for c in range(nc):
        inf_c[c][n] = jnp.zeros((2 * CHUNKS[c], HD), jnp.bfloat16)
    run_s[n] = jnp.zeros(run_s.shape[1:], jnp.float32)
    for c in range(AHEAD, nc):
        stage_keys(c)
    req_vector.wait()
    lane_n = lax.broadcasted_iota(jnp.int32, (n, LANES), 1)
    row_n = lax.broadcasted_iota(jnp.int32, (n, LANES), 0)
    code_col = jnp.sum(jnp.where((lane_n == me) & (row_n > me), reqs_v[...], 0), axis=1, keepdims=True)
    code_col = jnp.where(row_n[:, :1] > me, code_col, -1)
    item_col = jnp.where(code_col >= 0, code_col % items, items)
    item_full = jnp.broadcast_to(item_col, (n, LANES))
    key_full = item_full * LANES + row_n
    diag = row_n == lane_n
    item_row = jnp.sum(jnp.where(diag, item_full, 0), axis=0, keepdims=True)
    item_row = jnp.where(lane_n[:1] < n, item_row, items)
    key_row = jnp.sum(jnp.where(diag, key_full, 0), axis=0, keepdims=True)
    key_row = jnp.where(lane_n[:1] < n, key_row, LANES * LANES)
    rank_col = jnp.sum(jnp.where(key_row < key_full, 1, 0), axis=1, keepdims=True)
    order_row = jnp.sum(jnp.where(rank_col == lane_n, row_n, 0), axis=0, keepdims=True)
    upto_row = jnp.sum(jnp.where(item_full <= lane_n, 1, 0), axis=0, keepdims=True)
    below_row = jnp.sum(jnp.where(item_full < lane_n, 1, 0), axis=0, keepdims=True)
    lead_col = jnp.sum(jnp.where(item_row < item_full, 1, 0), axis=1, keepdims=True)
    lead_col = jnp.where(lead_col == rank_col, 1, 0)
    fresh_row = jnp.sum(jnp.where(rank_col == lane_n, lead_col, 0), axis=0, keepdims=True)
    tab_v[1:2, :] = order_row
    tab_v[2:3, :] = jnp.maximum(upto_row - 1, 0)
    tab_v[3:4, :] = jnp.where(upto_row > below_row, 1, 0)
    tab_v[4:5, :] = fresh_row
    tab_copy = pltpu.make_async_copy(tab_v, tab_s, misc_sem.at[0])
    tab_copy.start()

    pltpu.make_async_copy(q_s, q_s, load_sem.at[2]).wait()
    lax.fori_loop(0, items, own_block, 0)

    for c in range(nc):
        wait_keys(c)
        chunk_grads(c)
        stage_grads(c)
        send(c + AHEAD)
    tab_copy.wait()

    def finish_query(index, _):
        b = index // (KVH * GROUP)
        i = index % (KVH * GROUP)
        item = b * KVH + i // GROUP
        cols = pl.ds(pl.multiple_of((i % GROUP) * BLK, BLK), BLK)
        rows = pl.ds(pl.multiple_of(b * BLK, BLK), BLK)
        part = dq_s[item, :, cols].T * SCALE
        gq_s[rows, pl.ds(pl.multiple_of(i * HD, HD), HD)] = part.astype(jnp.bfloat16)
        return _

    lax.fori_loop(0, items * GROUP, finish_query, 0)
    out_q = pltpu.make_async_copy(gq_s, gq_hbm, misc_sem.at[1])
    out_q.start()

    for c in range(nc):
        wait_grads(c)
        fold(c)
    out_k = pltpu.make_async_copy(gk_s, gk_hbm, misc_sem.at[2])
    out_v = pltpu.make_async_copy(gv_s, gv_hbm, misc_sem.at[3])
    out_k.start()
    out_v.start()

    def wait_req_sent(peer, _):
        req_copy(peer, me).wait_send()
        return _

    lax.fori_loop(0, me, wait_req_sent, 0)
    wait_sent(nc + AHEAD - 2)
    wait_sent(nc + AHEAD - 1)
    out_q.wait()
    out_k.wait()
    out_v.wait()


def shards(query, keys, values, output, grad_out, logsumexp, selected):
    bulk = lax.axis_size("bulk")
    n = lax.axis_size("ctx") * bulk
    tokens = query.shape[0]
    local_blocks = tokens // BLK
    items = local_blocks * KVH
    per_device = items * TOPK
    chosen = selected.reshape(per_device)
    slots = jnp.arange(per_device, dtype=jnp.int32)
    code = slots * items + chosen % local_blocks * KVH + slots // TOPK % KVH
    owners = jnp.where(chosen >= 0, chosen // local_blocks, -1)
    matches = owners[:, None] == jnp.arange(LANES, dtype=jnp.int32)[None, :]
    comb = jnp.max(jnp.where(matches, code[:, None], -1), axis=0)
    lse = jnp.transpose(logsumexp.reshape(local_blocks, BLK, KVH * GROUP), (0, 2, 1))
    bf16, f32, i32 = jnp.bfloat16, jnp.float32, jnp.int32
    nc = len(CHUNKS)
    widest = max(CHUNKS)
    any_spec = pl.BlockSpec(memory_space=pl.ANY)
    vmem = pl.BlockSpec(memory_space=pltpu.VMEM)
    smem = pl.BlockSpec(memory_space=pltpu.SMEM)
    scratch = [
        pltpu.VMEM((items, GROUP * BLK, HD), bf16),
        pltpu.VMEM((items, GROUP * BLK, HD), bf16),
        pltpu.VMEM((items, GROUP * BLK, HD), bf16),
        pltpu.VMEM((items, 2 * BLK, HD), bf16),
        pltpu.VMEM((items, HD, GROUP * BLK), f32),
        pltpu.VMEM((items, 2 * BLK, HD), f32),
        pltpu.VMEM((local_blocks, LANES, BLK), f32),
        pltpu.VMEM((per_device, 2 * widest, HD), bf16),
        pltpu.VMEM((n + 1, 2 * widest, HD), f32),
        pltpu.VMEM(query.shape, bf16),
        pltpu.VMEM(keys.shape, bf16),
        pltpu.VMEM(values.shape, bf16),
        pltpu.SMEM((n, LANES), i32),
        pltpu.VMEM((n, LANES), i32),
        pltpu.VMEM((8, LANES), i32),
        pltpu.SMEM((8, LANES), i32),
        *[pltpu.VMEM((n, 2 * size, HD), bf16) for size in CHUNKS],
        *[pltpu.VMEM((n, 2 * size, HD), bf16) for size in CHUNKS],
        *[pltpu.VMEM((n + 1, 2 * size, HD), bf16) for size in CHUNKS],
        *[pltpu.VMEM((n, 2 * size, HD), bf16) for size in CHUNKS],
        pltpu.SemaphoreType.DMA((4,)),
        pltpu.SemaphoreType.DMA((5,)),
        pltpu.SemaphoreType.DMA((2, n)),
        pltpu.SemaphoreType.DMA((n,)),
        pltpu.SemaphoreType.DMA((n,)),
        pltpu.SemaphoreType.DMA((nc, n)),
    ]
    return pl.pallas_call(
        functools.partial(kernel, n, bulk, local_blocks),
        out_shape=(
            jax.ShapeDtypeStruct(query.shape, bf16),
            jax.ShapeDtypeStruct(keys.shape, bf16),
            jax.ShapeDtypeStruct(values.shape, bf16),
        ),
        in_specs=[any_spec] * 5 + [vmem, smem, smem],
        out_specs=(any_spec,) * 3,
        scratch_shapes=scratch,
        compiler_params=pltpu.CompilerParams(
            collective_id=0, has_side_effects=True, vmem_limit_bytes=63_000_000
        ),
        name="block_sparse_backward",
    )(query, grad_out, output, keys, values, lse, comb[None, :], chosen)


def solution(mesh):
    rows = P(("ctx", "bulk"), None)
    in_specs = (rows,) * 6 + (P(("ctx", "bulk"), None, None),)
    return jax.shard_map(
        shards, mesh=mesh, in_specs=in_specs, out_specs=(rows,) * 3, check_vma=False
    )
```

```python
import functools

import jax
import jax.numpy as jnp
from jax import lax
from jax.experimental import pallas as pl
from jax.experimental.pallas import tpu as pltpu
from jax.sharding import PartitionSpec as P

HD = 128
KVH = 8
GROUP = 5
BLK = 128
TOPK = 3
LANES = 128
CHUNKS = (16,) * 8
AHEAD = 2
STRIDE = 37
UNROLL = 4
LOG2E = 1.4426950408889634
SCALE = HD ** (-0.5)
MESH = pl.DeviceIdType.MESH
NT = (((1,), (1,)), ((), ()))
TN = (((0,), (0,)), ((), ()))
NN = (((1,), (0,)), ((), ()))


def dot(a, b, dims):
    return lax.dot_general(a, b, dims, preferred_element_type=jnp.float32)


def kernel(n, bulk, local_blocks, *refs):
    nc = len(CHUNKS)
    starts = [sum(CHUNKS[:c]) for c in range(nc)]
    items = local_blocks * KVH
    rows_q = GROUP * BLK
    refs = list(refs)

    def take(count):
        out = refs[:count]
        del refs[:count]
        return out

    q_hbm, g_hbm, o_hbm, k_hbm, v_hbm, lse_ref, comb_s, sel_s = take(8)
    gq_hbm, gk_hbm, gv_hbm = take(3)
    q_s, g_s, o_s, kv_s, dq_s, own_s, delta_s, part_s, run_s, gq_s, gk_s, gv_s = take(12)
    reqs_s, reqs_v, tab_v, tab_s = take(4)
    out_c = take(nc)
    inf_c = take(nc)
    inb_c = take(nc)
    load_sem, misc_sem, send_sem, req_send, req_recv, recv_sem = take(6)

    me = lax.axis_index("ctx") * bulk + lax.axis_index("bulk")

    def place(peer):
        return (peer // bulk, peer % bulk)

    barrier = pltpu.get_barrier_semaphore()

    def greet(step, _):
        peer = (me + step) % n
        pl.semaphore_signal(barrier, inc=1, device_id=place(peer), device_id_type=MESH)
        return _

    lax.fori_loop(1, n, greet, 0)

    def load_heads(index, _):
        b = index // (KVH * GROUP)
        i = index % (KVH * GROUP)
        src = (pl.ds(pl.multiple_of(b * BLK, BLK), BLK), pl.ds(pl.multiple_of(i * HD, HD), HD))
        at = pl.ds(pl.multiple_of((i % GROUP) * BLK, BLK), BLK)
        item = b * KVH + i // GROUP
        pltpu.make_async_copy(g_hbm.at[src], g_s.at[item, at], load_sem.at[0]).start()
        pltpu.make_async_copy(o_hbm.at[src], o_s.at[item, at], load_sem.at[1]).start()
        pltpu.make_async_copy(q_hbm.at[src], q_s.at[item, at], load_sem.at[2]).start()
        return _

    def load_kv(index, _):
        b = index // KVH
        h = index % KVH
        src = (pl.ds(pl.multiple_of(b * BLK, BLK), BLK), pl.ds(pl.multiple_of(h * HD, HD), HD))
        pltpu.make_async_copy(k_hbm.at[src], kv_s.at[index, pl.ds(0, BLK)], load_sem.at[3]).start()
        pltpu.make_async_copy(v_hbm.at[src], kv_s.at[index, pl.ds(BLK, BLK)], load_sem.at[3]).start()
        return _

    lax.fori_loop(0, items, load_kv, 0)
    lax.fori_loop(0, items * GROUP, load_heads, 0)
    pl.semaphore_wait(barrier, n - 1)

    def req_copy(peer, row):
        return pltpu.make_async_remote_copy(
            src_ref=comb_s,
            dst_ref=reqs_s.at[pl.ds(row, 1)],
            send_sem=req_send.at[peer],
            recv_sem=req_recv.at[row],
            device_id=place(peer),
            device_id_type=MESH,
        )

    def send_req(peer, _):
        req_copy(peer, me).start()
        return _

    lax.fori_loop(0, me, send_req, 0)

    pltpu.make_async_copy(g_s, g_s, load_sem.at[0]).wait()
    pltpu.make_async_copy(o_s, o_s, load_sem.at[1]).wait()
    lane = lax.broadcasted_iota(jnp.int32, (BLK, LANES), 1)
    row = lax.broadcasted_iota(jnp.int32, (BLK, LANES), 0)
    for b in range(local_blocks):

        def one_delta(i, acc):
            item = b * KVH + i // GROUP
            at = pl.ds(pl.multiple_of((i % GROUP) * BLK, BLK), BLK)
            prod = g_s[item, at, :].astype(jnp.float32) * o_s[item, at, :].astype(jnp.float32)
            return jnp.where(lane == i, jnp.sum(prod, axis=1, keepdims=True), acc)

        acc = lax.fori_loop(0, KVH * GROUP, one_delta, jnp.zeros((BLK, LANES), jnp.float32))
        delta_s[b] = acc.T

    def wait_req(peer, _):
        req_copy(peer, peer).wait_recv()
        return _

    lax.fori_loop(me + 1, n, wait_req, 0)

    pltpu.make_async_copy(kv_s, kv_s, load_sem.at[3]).wait()

    def data_copy(c, peer, source, box):
        return pltpu.make_async_remote_copy(
            src_ref=out_c[c].at[peer],
            dst_ref=box[c].at[source],
            send_sem=send_sem.at[c],
            recv_sem=recv_sem.at[c, source],
            device_id=place(peer),
            device_id_type=MESH,
        )

    stride = STRIDE if n == 128 else 1

    def stage_keys(c):
        size, at = CHUNKS[c], starts[c]

        def one(peer, _):
            want = lax.rem(jnp.maximum(reqs_s[peer, me], 0), items)
            out_c[c][peer, 0:size, :] = kv_s[want, at : at + size, :]
            out_c[c][peer, size : 2 * size, :] = kv_s[want, BLK + at : BLK + at + size, :]
            return _

        lax.fori_loop(me + 1, n, one, 0)

    def send(keys_c, grads_c):
        def one(step, _):
            peer = (me + step * stride) % n
            if keys_c is not None:

                @pl.when(peer > me)
                def go_keys():
                    data_copy(keys_c, peer, me, inf_c).start()

            if grads_c is not None:

                @pl.when(peer < me)
                def go_grads():
                    data_copy(grads_c, peer, me, inb_c).start()

            return _

        lax.fori_loop(1, n, one, 0)

    def stage_grads(c):
        def one(peer, _):
            slot = lax.div(jnp.maximum(comb_s[0, peer], 0), items)
            out_c[c][peer] = part_s[slot, 0 : 2 * CHUNKS[c], :]
            return _

        lax.fori_loop(0, me, one, 0)

    def wait_keys(c):
        def one(peer, _):
            data_copy(c, peer, peer, inf_c).wait_recv()
            return _

        lax.fori_loop(0, me, one, 0)

    def wait_grads(c):
        def one(peer, _):
            data_copy(c, peer, peer, inb_c).wait_recv()
            return _

        lax.fori_loop(me + 1, n, one, 0)

    def rows_of(item, box):
        b, h = item // KVH, item % KVH
        return jnp.concatenate([box[b, pl.ds(h * GROUP + g, 1), :] for g in range(GROUP)], axis=1)

    def attend(item, key_set, value_set, mask):
        queries, grads = q_s[item], g_s[item]
        scores = dot(key_set, queries, NT)
        probs32 = jnp.exp2(scores * (SCALE * LOG2E) - rows_of(item, lse_ref) * LOG2E)
        if mask is not None:
            probs32 = jnp.where(mask, probs32, 0.0)
        dprobs = dot(value_set, grads, NT)
        dscores = (probs32 * (dprobs - rows_of(item, delta_s))).astype(jnp.bfloat16)
        value_part = dot(probs32.astype(jnp.bfloat16), grads, NN)
        key_part = dot(dscores, queries, NN)
        return key_part, value_part, dot(key_set, dscores, TN)

    def own_block(item, _):
        key_at = lax.broadcasted_iota(jnp.int32, (BLK, rows_q), 0)
        query_at = lax.broadcasted_iota(jnp.int32, (BLK, rows_q), 1) % BLK
        key_part, value_part, query_part = attend(
            item, kv_s[item, 0:BLK, :], kv_s[item, BLK : 2 * BLK, :], key_at <= query_at
        )
        own_s[item, 0:BLK, :] = key_part
        own_s[item, BLK : 2 * BLK, :] = value_part
        dq_s[item] = query_part
        return _

    def chunk_grads(c):
        size = CHUNKS[c]

        def one(item, _):
            sets = []
            for s in range(TOPK):
                chosen = sel_s[item * TOPK + s]
                owner = jnp.where(chosen >= 0, chosen // local_blocks, n)
                sets.append(inf_c[c][owner])
            key_set = jnp.concatenate([x[:size] for x in sets], axis=0)
            value_set = jnp.concatenate([x[size:] for x in sets], axis=0)
            key_part, value_part, query_part = attend(item, key_set, value_set, None)
            for s in range(TOPK):
                at = slice(s * size, (s + 1) * size)
                part_s[item * TOPK + s, 0:size, :] = key_part[at].astype(jnp.bfloat16)
                part_s[item * TOPK + s, size : 2 * size, :] = value_part[at].astype(jnp.bfloat16)
            dq_s[item] += query_part
            return _

        lax.fori_loop(0, items, one, 0)

    def fold(c):
        size, at = CHUNKS[c], starts[c]

        def scan(k, acc):
            source = tab_s[1, k]
            acc = jnp.where(tab_s[4, k] > 0, 0.0, acc) + inb_c[c][source].astype(jnp.float32)
            run_s[k, 0 : 2 * size, :] = acc
            return acc

        lax.fori_loop(0, n, scan, jnp.zeros((2 * size, HD), jnp.float32), unroll=UNROLL)

        def finish(item, _):
            last = jnp.where(tab_s[3, item] > 0, tab_s[2, item], n)
            total = run_s[last, 0 : 2 * size, :]
            b, h = item // KVH, item % KVH
            rows = pl.ds(pl.multiple_of(b * BLK + at, 16), size)
            cols = pl.ds(pl.multiple_of(h * HD, HD), HD)
            key_sum = own_s[item, at : at + size, :] + total[:size]
            value_sum = own_s[item, BLK + at : BLK + at + size, :] + total[size:]
            gk_s[rows, cols] = (key_sum * SCALE).astype(jnp.bfloat16)
            gv_s[rows, cols] = value_sum.astype(jnp.bfloat16)
            return _

        lax.fori_loop(0, items, finish, 0, unroll=UNROLL)

    for c in range(AHEAD):
        stage_keys(c)
        send(c, None)
    req_vector = pltpu.make_async_copy(reqs_s, reqs_v, misc_sem.at[4])
    req_vector.start()
    for c in range(nc):
        inf_c[c][n] = jnp.zeros((2 * CHUNKS[c], HD), jnp.bfloat16)
    run_s[n] = jnp.zeros(run_s.shape[1:], jnp.float32)
    for c in range(AHEAD, nc):
        stage_keys(c)
    req_vector.wait()
    lane_n = lax.broadcasted_iota(jnp.int32, (n, LANES), 1)
    row_n = lax.broadcasted_iota(jnp.int32, (n, LANES), 0)
    code_col = jnp.sum(jnp.where((lane_n == me) & (row_n > me), reqs_v[...], 0), axis=1, keepdims=True)
    code_col = jnp.where(row_n[:, :1] > me, code_col, -1)
    item_col = jnp.where(code_col >= 0, code_col % items, items)
    item_full = jnp.broadcast_to(item_col, (n, LANES))
    key_full = item_full * LANES + row_n
    diag = row_n == lane_n
    item_row = jnp.sum(jnp.where(diag, item_full, 0), axis=0, keepdims=True)
    item_row = jnp.where(lane_n[:1] < n, item_row, items)
    key_row = jnp.sum(jnp.where(diag, key_full, 0), axis=0, keepdims=True)
    key_row = jnp.where(lane_n[:1] < n, key_row, LANES * LANES)
    rank_col = jnp.sum(jnp.where(key_row < key_full, 1, 0), axis=1, keepdims=True)
    order_row = jnp.sum(jnp.where(rank_col == lane_n, row_n, 0), axis=0, keepdims=True)
    upto_row = jnp.sum(jnp.where(item_full <= lane_n, 1, 0), axis=0, keepdims=True)
    below_row = jnp.sum(jnp.where(item_full < lane_n, 1, 0), axis=0, keepdims=True)
    lead_col = jnp.sum(jnp.where(item_row < item_full, 1, 0), axis=1, keepdims=True)
    lead_col = jnp.where(lead_col == rank_col, 1, 0)
    fresh_row = jnp.sum(jnp.where(rank_col == lane_n, lead_col, 0), axis=0, keepdims=True)
    tab_v[1:2, :] = order_row
    tab_v[2:3, :] = jnp.maximum(upto_row - 1, 0)
    tab_v[3:4, :] = jnp.where(upto_row > below_row, 1, 0)
    tab_v[4:5, :] = fresh_row
    tab_copy = pltpu.make_async_copy(tab_v, tab_s, misc_sem.at[0])
    tab_copy.start()

    pltpu.make_async_copy(q_s, q_s, load_sem.at[2]).wait()
    lax.fori_loop(0, items, own_block, 0)

    for c in range(nc):
        wait_keys(c)
        chunk_grads(c)
        stage_grads(c)
        send(c + AHEAD if c + AHEAD < nc else None, c)
    tab_copy.wait()

    def finish_query(index, _):
        b = index // (KVH * GROUP)
        i = index % (KVH * GROUP)
        item = b * KVH + i // GROUP
        cols = pl.ds(pl.multiple_of((i % GROUP) * BLK, BLK), BLK)
        rows = pl.ds(pl.multiple_of(b * BLK, BLK), BLK)
        part = dq_s[item, :, cols].T * SCALE
        gq_s[rows, pl.ds(pl.multiple_of(i * HD, HD), HD)] = part.astype(jnp.bfloat16)
        return _

    lax.fori_loop(0, items * GROUP, finish_query, 0)
    out_q = pltpu.make_async_copy(gq_s, gq_hbm, misc_sem.at[1])
    out_q.start()

    for c in range(nc):
        wait_grads(c)
        fold(c)
    out_k = pltpu.make_async_copy(gk_s, gk_hbm, misc_sem.at[2])
    out_v = pltpu.make_async_copy(gv_s, gv_hbm, misc_sem.at[3])
    out_k.start()
    out_v.start()

    def wait_req_sent(peer, _):
        req_copy(peer, me).wait_send()
        return _

    lax.fori_loop(0, me, wait_req_sent, 0)
    for c in range(nc):
        sent = out_c[c].at[pl.ds(0, n - 1)]
        pltpu.make_async_copy(sent, sent, send_sem.at[c]).wait()
    out_q.wait()
    out_k.wait()
    out_v.wait()


def shards(query, keys, values, output, grad_out, logsumexp, selected):
    bulk = lax.axis_size("bulk")
    n = lax.axis_size("ctx") * bulk
    tokens = query.shape[0]
    local_blocks = tokens // BLK
    items = local_blocks * KVH
    per_device = items * TOPK
    chosen = selected.reshape(per_device)
    slots = jnp.arange(per_device, dtype=jnp.int32)
    code = slots * items + chosen % local_blocks * KVH + slots // TOPK % KVH
    owners = jnp.where(chosen >= 0, chosen // local_blocks, -1)
    matches = owners[:, None] == jnp.arange(LANES, dtype=jnp.int32)[None, :]
    comb = jnp.max(jnp.where(matches, code[:, None], -1), axis=0)
    lse = jnp.transpose(logsumexp.reshape(local_blocks, BLK, KVH * GROUP), (0, 2, 1))
    bf16, f32, i32 = jnp.bfloat16, jnp.float32, jnp.int32
    nc = len(CHUNKS)
    widest = max(CHUNKS)
    any_spec = pl.BlockSpec(memory_space=pl.ANY)
    vmem = pl.BlockSpec(memory_space=pltpu.VMEM)
    smem = pl.BlockSpec(memory_space=pltpu.SMEM)
    scratch = [
        pltpu.VMEM((items, GROUP * BLK, HD), bf16),
        pltpu.VMEM((items, GROUP * BLK, HD), bf16),
        pltpu.VMEM((items, GROUP * BLK, HD), bf16),
        pltpu.VMEM((items, 2 * BLK, HD), bf16),
        pltpu.VMEM((items, HD, GROUP * BLK), f32),
        pltpu.VMEM((items, 2 * BLK, HD), f32),
        pltpu.VMEM((local_blocks, LANES, BLK), f32),
        pltpu.VMEM((per_device, 2 * widest, HD), bf16),
        pltpu.VMEM((n + 1, 2 * widest, HD), f32),
        pltpu.VMEM(query.shape, bf16),
        pltpu.VMEM(keys.shape, bf16),
        pltpu.VMEM(values.shape, bf16),
        pltpu.SMEM((n, LANES), i32),
        pltpu.VMEM((n, LANES), i32),
        pltpu.VMEM((8, LANES), i32),
        pltpu.SMEM((8, LANES), i32),
        *[pltpu.VMEM((n, 2 * size, HD), bf16) for size in CHUNKS],
        *[pltpu.VMEM((n + 1, 2 * size, HD), bf16) for size in CHUNKS],
        *[pltpu.VMEM((n, 2 * size, HD), bf16) for size in CHUNKS],
        pltpu.SemaphoreType.DMA((4,)),
        pltpu.SemaphoreType.DMA((5,)),
        pltpu.SemaphoreType.DMA((nc,)),
        pltpu.SemaphoreType.DMA((n,)),
        pltpu.SemaphoreType.DMA((n,)),
        pltpu.SemaphoreType.DMA((nc, n)),
    ]
    return pl.pallas_call(
        functools.partial(kernel, n, bulk, local_blocks),
        out_shape=(
            jax.ShapeDtypeStruct(query.shape, bf16),
            jax.ShapeDtypeStruct(keys.shape, bf16),
            jax.ShapeDtypeStruct(values.shape, bf16),
        ),
        in_specs=[any_spec] * 5 + [vmem, smem, smem],
        out_specs=(any_spec,) * 3,
        scratch_shapes=scratch,
        compiler_params=pltpu.CompilerParams(
            collective_id=0, has_side_effects=True, vmem_limit_bytes=63_000_000
        ),
        name="block_sparse_backward",
    )(query, grad_out, output, keys, values, lse, comb[None, :], chosen)


def solution(mesh):
    rows = P(("ctx", "bulk"), None)
    in_specs = (rows,) * 6 + (P(("ctx", "bulk"), None, None),)
    return jax.shard_map(
        shards, mesh=mesh, in_specs=in_specs, out_specs=(rows,) * 3, check_vma=False
    )
```
